32 devices in a mesh: batch: 16 (over z, x, core), seq: 2 (over y).
Axes of the slice: x: 2, y: 2, z: 4, core: 2. Of those that a mesh axis runs over, the one named last changes fastest.
Arguments:
- tokens: bfloat16 [16, 1024, 2560], P('batch', 'seq'), may hold values from -6 to 6
- attn_in: bfloat16 [16, 1024, 2560], P('batch', 'seq'), may hold values from -6 to 6
- lengths: int32 [16], P('batch'), may hold values from 256 to 1024
- norm_gain: float32 [2560], replicated, may hold values from 0.5 to 1.5
- attn_gain: float32 [2560], replicated, may hold values from 0.5 to 1.5
- w_x: bfloat16 [2560, 2560], P(('batch', 'seq')), may hold values from -0.125 to 0.125
- conv_w: float32 [4, 2560], replicated, may hold values from -3 to 3
- w_a: bfloat16 [10, 256, 256], replicated, may hold values from -0.375 to 0.375
- w_i: bfloat16 [10, 256, 256], replicated, may hold values from -0.375 to 0.375
- lru_decay: float32 [2560], replicated, may hold values from 4 to 20
- w_kv: bfloat16 [2560, 512], replicated, may hold values from -0.125 to 0.125
Outputs:
- lru_state: float32 [16, 2560], P('batch', 'seq')
- conv_state: bfloat16 [16, 3, 2560], P('batch', None, 'seq')
- kv_cache: bfloat16 [16, 2048, 512], P('batch', None, 'seq')
The draws below stay inside these ranges and needn't reach their ends.
Inputs may be any that keep to these rules, and one draw needn't show every extreme that they name: `lengths`: positions from a prompt's length on are padding.
All inputs are finite; a program needn't handle non-finite values.
Results may differ from the reference program's by a relative error of at most 0.0051.
Values may be sent and summed in bfloat16 or wider, within the bound.
No kernel may reach another device: no remote copies, remote signals or barrier semaphores. Data moves between devices by JAX's collectives and lax.ppermute only.
A program may use at most 128 MiB of HBM per device.

```python
import jax
import jax.numpy as jnp
from jax import lax

D = 2560
H = 10
HD = 256
W = 2048
SEQ = 1024
PROMPTS = 16


def draw_lru_decay(key, part):
    pick_key = jax.random.fold_in(key, 11)
    slow_key = jax.random.fold_in(key, 12)
    fast_key = jax.random.fold_in(key, 13)
    share = 50
    fast_mask = jax.random.randint(pick_key, (D,), 0, 100) < share
    slow_value = jnp.log(8.0 * SEQ / jax.random.uniform(slow_key, (D,), jnp.float32, 0.2, 1.0))
    fast_value = jnp.log(jax.random.uniform(fast_key, (D,), jnp.float32, 120.0, 200.0))
    return jnp.where(fast_mask, fast_value, slow_value).astype(jnp.float32)


def place_ends(array, own_key, smallest, largest):
    index_at = [jax.random.randint(jax.random.fold_in(own_key, axis), (), 0, length) for axis, length in enumerate(array.shape)]
    widest = array.shape.index(max(array.shape))
    beside = index_at[:widest] + [(index_at[widest] + 1) % array.shape[widest]] + index_at[widest + 1:]
    return array.at[tuple(index_at)].set(smallest).at[tuple(beside)].set(largest)


def shard_levels(stream_key, shape, pieces, smallest, largest):
    def one(axis_at, blocks):
        heights = jax.random.uniform(jax.random.fold_in(jax.random.fold_in(stream_key, 6), axis_at), (blocks,), jnp.float32, smallest / len(pieces), largest / len(pieces))
        return jnp.repeat(jnp.exp(heights), shape[axis_at] // blocks).reshape((-1,) + (1,) * (len(shape) - axis_at - 1))

    loudness = one(*pieces[0])
    for cut in pieces[1:]:
        loudness = loudness * one(*cut)
    return loudness


def noise(rng, dims, spread, reach, pieces=(), kind=jnp.bfloat16):
    result = jax.random.normal(rng, dims, jnp.float32) * spread
    if len(pieces) > 0:
        result = shard_levels(rng, dims, pieces, -0.22, 0.18) * result
    return jnp.clip(result, min=-reach, max=reach).astype(kind)


def setup_inputs(seed: int = 0) -> dict:
    key_list = jax.random.split(jax.random.key(seed), 12)
    return {
        "tokens": noise(key_list[0], (PROMPTS, SEQ, D), 1.0, 6.0, ((0, 16), (1, 2))),
        "attn_in": noise(key_list[1], (PROMPTS, SEQ, D), 1.0, 6.0, ((0, 16), (1, 2))),
        "lengths": place_ends(jax.random.randint(key_list[2], (PROMPTS,), SEQ // 4, SEQ + 1), jax.random.fold_in(key_list[2], 1), SEQ // 4, SEQ).astype(jnp.int32),
        "norm_gain": jnp.clip(1.0 + 0.1 * jax.random.normal(key_list[3], (D,), jnp.float32), 0.5, 1.5),
        "attn_gain": jnp.clip(1.0 + 0.1 * jax.random.normal(key_list[4], (D,), jnp.float32), 0.5, 1.5),
        "w_x": noise(key_list[5], (D, D), D ** -0.5, 0.125, ((0, 32),)),
        "conv_w": noise(key_list[6], (4, D), 0.5, 3.0, (), jnp.float32),
        "w_a": noise(key_list[7], (H, HD, HD), HD ** -0.5, 0.375),
        "w_i": noise(key_list[8], (H, HD, HD), HD ** -0.5, 0.375),
        "lru_decay": draw_lru_decay(jax.random.fold_in(key_list[11], 71), 0),
        "w_kv": noise(key_list[10], (D, 2 * HD), D ** -0.5, 0.125),
    }


def rms_norm(values, gain_vec):
    widened = values.astype(jnp.float32)
    inverse = lax.rsqrt(lax.optimization_barrier(jnp.mean(widened * widened, axis=-1, keepdims=True)) + 1e-06)
    return (widened * inverse * gain_vec).astype(jnp.bfloat16)

def rotate_keys(key_rows, positions):
    quarter = key_rows.shape[-1] // 4
    spacing = jnp.exp(-jnp.log(10000.0) * jnp.arange(quarter, dtype=jnp.float32) / quarter)
    angles = positions.astype(jnp.float32)[:, None] * spacing[None, :]
    cosine_rows = jnp.cos(angles)
    sine_rows = jnp.sin(angles)
    first_part = key_rows[:, :quarter]
    second_part = key_rows[:, quarter:2 * quarter]
    return jnp.concatenate([first_part * cosine_rows - second_part * sine_rows, second_part * cosine_rows + first_part * sine_rows, key_rows[:, 2 * quarter:]], axis=1)

def one_prompt(norm_gain, attn_gain, w_x, conv_w, w_a, w_i, lru_decay, w_kv, tokens, attn_in, length):
    seq_len = tokens.shape[0]
    normed = rms_norm(tokens, norm_gain)
    x_proj = jnp.dot(normed, w_x, preferred_element_type=jnp.float32).astype(jnp.bfloat16)
    padded = jnp.concatenate([jnp.zeros((3, D), jnp.bfloat16), x_proj], axis=0)
    conv_sum = conv_w[0] * padded[0:seq_len].astype(jnp.float32)
    for offset in range(1, 4):
        conv_sum = conv_sum + conv_w[offset] * padded[offset:offset + seq_len].astype(jnp.float32)
    x_conv = conv_sum.astype(jnp.bfloat16)
    head_rows = x_conv.astype(jnp.float32).reshape(seq_len, H, HD)
    gate_a = jnp.einsum('lhk,hkj->lhj', head_rows, w_a.astype(jnp.float32)).reshape(seq_len, D)
    gate_i = jnp.einsum('lhk,hkj->lhj', head_rows, w_i.astype(jnp.float32)).reshape(seq_len, D)
    positions = jnp.arange(seq_len, dtype=jnp.int32)
    valid_row = (positions < length).astype(jnp.float32)[:, None]
    log_rate = -8.0 * jax.nn.softplus(-lru_decay) * jax.nn.sigmoid(gate_a)
    keep_rate = jnp.exp(log_rate * valid_row)
    push_term = jnp.sqrt(-jnp.expm1(2.0 * log_rate)) * jax.nn.sigmoid(gate_i) * x_conv.astype(jnp.float32) * valid_row

    def advance(carried, step_pair):
        return (step_pair[0] * carried + step_pair[1], None)
    lru_state = lax.scan(advance, jnp.zeros((D,), jnp.float32), (keep_rate, push_term))[0]
    conv_state = lax.dynamic_slice_in_dim(padded, length.astype(jnp.int32), 3, 0)
    attn_normed = rms_norm(attn_in, attn_gain)
    kv_full = jnp.dot(attn_normed, w_kv, preferred_element_type=jnp.float32)
    kv_rows = jnp.concatenate([rotate_keys(kv_full[:, :HD], positions), kv_full[:, HD:]], axis=1).astype(jnp.bfloat16)
    in_window = ((positions >= length - W) & (positions < length)).astype(jnp.float32)[:, None]
    masked = kv_rows.astype(jnp.float32) * in_window
    lap_count = -(-seq_len // W)
    masked = jnp.concatenate([masked, jnp.zeros((lap_count * W - seq_len, 2 * HD), jnp.float32)], axis=0)
    kv_cache = lax.optimization_barrier(jnp.sum(masked.reshape(lap_count, W, 2 * HD), axis=0)).astype(jnp.bfloat16)
    return (lru_state, conv_state, kv_cache)

def reference(tokens, attn_in, lengths, norm_gain, attn_gain, w_x, conv_w, w_a, w_i, lru_decay, w_kv):

    def per_prompt(inputs):
        return one_prompt(norm_gain, attn_gain, w_x, conv_w, w_a, w_i, lru_decay, w_kv, inputs[0], inputs[1], inputs[2])
    lru_state, conv_state, kv_cache = lax.map(per_prompt, (tokens, attn_in, lengths))
    return (lru_state, conv_state, kv_cache)
```

```python
import functools

import jax
import jax.numpy as jnp
from jax import lax
from jax.experimental import pallas as pl
from jax.experimental.pallas import tpu as pltpu
from jax.sharding import PartitionSpec as P

H = 10
HD = 256
W = 2048
TAPS = 4
SUB = 8
HALO = 16


def prep_kernel(tok_ref, halo_ref, gain_ref, out_ref, flat_ref):
    rows = tok_ref.shape[0]
    gain = gain_ref[...]

    def norm(values):
        widened = values.astype(jnp.float32)
        inverse = lax.rsqrt(jnp.mean(widened * widened, axis=-1, keepdims=True) + 1e-06)
        return (widened * inverse * gain).astype(jnp.bfloat16)

    chunk = 64

    def one(i, carry):
        at = pl.ds(pl.multiple_of(i * chunk, chunk), chunk)
        flat_ref[at, :] = norm(tok_ref[at, :])
        return carry

    lax.fori_loop(0, rows // chunk, one, 0)
    run = rows // SUB
    row = lax.broadcasted_iota(jnp.int32, (rows, rows), 0)
    col = lax.broadcasted_iota(jnp.int32, (rows, rows), 1)
    picked = ((row % SUB) * run + row // SUB == col).astype(jnp.bfloat16)
    out_ref[pl.ds(0, rows), :] = jnp.dot(
        picked, flat_ref[...], preferred_element_type=jnp.float32
    ).astype(jnp.bfloat16)
    out_ref[pl.ds(rows, HALO), :] = norm(halo_ref[...])


def main_kernel(
    scal_ref, own_ref, oth_ref, conv_ref, wa_ref, wi_ref, soft_ref, *rest, owners, seq_parts
):
    shard_refs = rest[: len(owners)]
    out_ref, w_ref, xs_ref, xc_ref, ga_ref, gi_ref = rest[len(owners) :]
    batch_at = scal_ref[0]
    seq_at = scal_ref[1]
    rows = own_ref.shape[0] - HALO
    run = rows // SUB
    core = batch_at % 2
    half_rows = shard_refs[0].shape[0] // 2
    cols = shard_refs[0].shape[1]
    heads = cols // HD
    pad = (TAPS - 1) * SUB

    for ref, (dz, dx, dy) in zip(shard_refs, owners):
        depth = scal_ref[4]
        z_at = lax.rem(batch_at // 4 + depth - dz, depth)
        x_at = (batch_at // 2 % 2 + dx) % 2
        y_at = (seq_at + dy) % 2
        for side in range(2):
            b_from = z_at * 4 + x_at * 2 + (core + side) % 2
            start = pl.multiple_of((b_from * seq_parts + y_at) * half_rows, 16)
            w_ref[pl.ds(start, half_rows), :] = ref[pl.ds(side * half_rows, half_rows), :]

    def head(h, carry):
        here = pl.ds(pl.multiple_of(h * HD, HD), HD)
        whole_head = core * heads + h
        there = pl.ds(pl.multiple_of(whole_head * HD, HD), HD)
        taps = conv_ref[:, there]
        soft = soft_ref[:, there]
        for p, n_ref in enumerate((own_ref, oth_ref)):
            xp = jnp.dot(n_ref[...], w_ref[:, here], preferred_element_type=jnp.float32)
            xp = xp.astype(jnp.bfloat16).astype(jnp.float32)
            xs_ref[p, pl.ds(pad, rows), :] = xp[:rows]
            for j in range(TAPS - 1):
                at = (run - (TAPS - 1) + j) * SUB
                late = rows + HALO - (TAPS - 1) + j
                xs_ref[p, pl.ds(j * SUB, SUB), :] = jnp.concatenate(
                    [xp[late : late + 1], xp[at : at + SUB - 1]], axis=0
                )
        for p in range(2):
            total = taps[0:1] * xs_ref[p, pl.ds(0, rows), :]
            for j in range(1, TAPS):
                total = total + taps[j : j + 1] * xs_ref[p, pl.ds(j * SUB, rows), :]
            xc_ref[p] = total.astype(jnp.bfloat16)
        for p in range(2):
            ga_ref[p] = jnp.dot(xc_ref[p], wa_ref[whole_head], preferred_element_type=jnp.float32)
            gi_ref[p] = jnp.dot(xc_ref[p], wi_ref[whole_head], preferred_element_type=jnp.float32)

        group = 4
        lane_step = lax.broadcasted_iota(jnp.int32, (SUB, HD), 0) * run

        def steps(i, state):
            new = []
            for p in range(2):
                keep_all, push_all = state[2 * p], state[2 * p + 1]
                at = pl.ds(pl.multiple_of(i * (group * SUB), group * SUB), group * SUB)
                rate = (-8.0 * soft) * jax.nn.sigmoid(ga_ref[p, at, :])
                keep = jnp.exp(rate)
                tan = jnp.tanh(rate)
                top = -2.0 * tan
                root = top * lax.rsqrt(jnp.maximum(top * (1.0 - tan), 1e-37))
                push = root * jax.nn.sigmoid(gi_ref[p, at, :]) * xc_ref[p, at, :].astype(jnp.float32)
                limit = scal_ref[2 + p] - seq_at * rows - i * group
                for g in range(group):
                    valid = lane_step < limit - g
                    k = jnp.where(valid, keep[g * SUB : (g + 1) * SUB], 1.0)
                    q = jnp.where(valid, push[g * SUB : (g + 1) * SUB], 0.0)
                    push_all = k * push_all + q
                    keep_all = k * keep_all
                new += [keep_all, push_all]
            return tuple(new)

        one = jnp.ones((SUB, HD), jnp.float32)
        zero = jnp.zeros((SUB, HD), jnp.float32)
        state = lax.fori_loop(0, run // group, steps, (one, zero, one, zero))
        for p in range(2):
            keep_all, push_all = state[2 * p], state[2 * p + 1]
            keep_one = keep_all[0:1]
            push_one = push_all[0:1]
            for s in range(1, SUB):
                push_one = keep_all[s : s + 1] * push_one + push_all[s : s + 1]
                keep_one = keep_all[s : s + 1] * keep_one
            picks = []
            for j in range(3):
                t = scal_ref[2 + p] - 3 + j - seq_at * rows
                inside = (t >= 0) & (t < rows)
                t = jnp.clip(t, 0, rows - 1)
                r = pad + t % run * SUB + t // run
                picks.append(jnp.where(inside, xs_ref[p, pl.ds(r, 1), :], 0.0))
            out_ref[p, :, here] = jnp.concatenate(
                [keep_one, push_one, *picks, jnp.zeros((3, HD), jnp.float32)], axis=0
            )
        return carry

    lax.fori_loop(0, heads, head, 0)


def in_vmem(count):
    return [pl.BlockSpec(memory_space=pltpu.VMEM)] * count


def shared_by_cores(
    tokens, attn_in, lengths, norm_gain, attn_gain, w_x, conv_w, w_a, w_i, lru_decay, w_kv
):
    local_len = tokens.shape[1]
    feature_dim = tokens.shape[2]
    batch_parts = lax.axis_size("batch")
    depth = batch_parts // 4
    batch_at = lax.axis_index("batch")
    seq_at = lax.axis_index("seq")
    core = batch_at % 2
    cols = feature_dim // 2

    core_swap = [(b, b ^ 1) for b in range(batch_parts)]
    x_swap = [(b, b ^ 2) for b in range(batch_parts)]

    def over_core(a):
        return lax.ppermute(a, "batch", core_swap)

    def over_x(a):
        return lax.ppermute(a, "batch", x_swap)

    def over_y(a):
        return lax.ppermute(a, "seq", [(0, 1), (1, 0)])

    def along_z(a, k):
        return lax.ppermute(a, "batch", [(b, (b + 4 * k) % batch_parts) for b in range(batch_parts)])

    mine = lax.dynamic_slice_in_dim(w_x, core * cols, cols, 1)
    theirs = over_core(lax.dynamic_slice_in_dim(w_x, (1 - core) * cols, cols, 1))
    shard = jnp.concatenate([mine, theirs], axis=0)

    order = [0] + [k for pair in zip(range(1, depth), range(depth - 1, 0, -1)) for k in pair]
    order = list(dict.fromkeys(order))
    planes = [shard] + [along_z(shard, k) for k in order[1:]]
    shards, owners = [], []
    for n, (k, plane) in enumerate(zip(order, planes)):
        beside_x = over_x(plane)
        beside_y = over_y(plane)
        across = over_y(beside_x) if n % 2 == 0 else over_x(beside_y)
        shards += [plane, beside_x, beside_y, across]
        owners += [(k, 0, 0), (k, 1, 0), (k, 0, 1), (k, 1, 1)]

    halo = lax.ppermute(tokens[0, local_len - HALO :], "seq", [(0, 1)])
    normed = pl.pallas_call(
        prep_kernel,
        out_shape=jax.ShapeDtypeStruct((local_len + HALO, feature_dim), jnp.bfloat16),
        in_specs=in_vmem(3),
        out_specs=pl.BlockSpec(memory_space=pltpu.VMEM),
        scratch_shapes=[pltpu.VMEM((local_len, feature_dim), jnp.bfloat16)],
        name="prep",
    )(tokens[0], halo, norm_gain[None])
    normed_other = over_core(normed)
    length_other = over_core(lengths)
    scalars = jnp.stack(
        [batch_at, seq_at, lengths[0], length_other[0], jnp.int32(depth)]
    ).astype(jnp.int32)
    soft = jax.nn.softplus(-lru_decay)[None]

    sums = pl.pallas_call(
        functools.partial(main_kernel, owners=tuple(owners), seq_parts=2),
        out_shape=jax.ShapeDtypeStruct((2, 8, cols), jnp.float32),
        in_specs=[pl.BlockSpec(memory_space=pltpu.SMEM)] + in_vmem(6 + len(shards)),
        out_specs=pl.BlockSpec(memory_space=pltpu.VMEM),
        scratch_shapes=[
            pltpu.VMEM((feature_dim, cols), jnp.bfloat16),
            pltpu.VMEM((2, local_len + (TAPS - 1) * SUB, HD), jnp.float32),
            pltpu.VMEM((2, local_len, HD), jnp.bfloat16),
            pltpu.VMEM((2, local_len, HD), jnp.float32),
            pltpu.VMEM((2, local_len, HD), jnp.float32),
        ],
        compiler_params=pltpu.CompilerParams(vmem_limit_bytes=48 * 1024 * 1024),
        name="layer",
    )(scalars, normed, normed_other, conv_w, w_a, w_i, soft, *shards)

    same = core == seq_at
    send_a = jnp.where(same, sums[0], sums[1])
    send_b = jnp.where(same, sums[1], sums[0])
    flat = [(b, s) for b in range(batch_parts) for s in range(2)]
    route_a = [(2 * b + s, 2 * (b // 2 * 2 + s) + b % 2) for b, s in flat]
    route_b = [(2 * b + s, 2 * (b // 2 * 2 + 1 - s) + b % 2) for b, s in flat]
    got_a = lax.ppermute(send_a, ("batch", "seq"), route_a)
    got_b = lax.ppermute(send_b, ("batch", "seq"), route_b)
    first = jnp.where(core == 0, got_a, got_b)
    second = jnp.where(core == 0, got_b, got_a)
    lru_state = second[0] * first[1] + second[1]
    decoded = (first[2:5] + second[2:5]).astype(jnp.bfloat16)

    positions = seq_at * local_len + jnp.arange(local_len, dtype=jnp.int32)
    kv_rows = local_kv(attn_in[0], attn_gain, w_kv, positions, lengths[0]).astype(jnp.bfloat16)
    kept = lax.dynamic_slice_in_dim(kv_rows, seq_at * HD, HD, 1)
    moved = over_y(lax.dynamic_slice_in_dim(kv_rows, (1 - seq_at) * HD, HD, 1))
    low = jnp.where(seq_at == 0, kept, moved)
    high = jnp.where(seq_at == 0, moved, kept)
    kv_cache = fold_window(jnp.concatenate([low, high], axis=0))
    return (lru_state[None], decoded[None], kv_cache[None])


def fold_window(rows):
    laps = -(-rows.shape[0] // W)
    padded = jnp.pad(rows, ((0, laps * W - rows.shape[0]), (0, 0)))
    return jnp.sum(padded.reshape(laps, W, rows.shape[1]).astype(jnp.float32), axis=0).astype(
        jnp.bfloat16
    )


def local_kv(rows, gain, w_kv, positions, length):
    attn_normed = rms_norm(rows, gain)
    kv_full = jnp.dot(attn_normed, w_kv, preferred_element_type=jnp.float32)
    kv_rows = jnp.concatenate(
        [rotate_keys(kv_full[:, :HD], positions), kv_full[:, HD:]], axis=1
    )
    in_window = ((positions >= length - W) & (positions < length))[:, None]
    return jnp.where(in_window, kv_rows, 0.0)


def passed_along(block, axis, distance):
    devices = range(lax.axis_size(axis))
    route = [(i - distance, i) for i in devices if i - distance in devices]
    return lax.ppermute(block, axis, route)


def rms_norm(values, gain_vec):
    widened = values.astype(jnp.float32)
    inverse = lax.rsqrt(jnp.mean(widened * widened, axis=-1, keepdims=True) + 1e-06)
    return (widened * inverse * gain_vec).astype(jnp.bfloat16)


def rotate_keys(key_rows, positions):
    quarter = key_rows.shape[-1] // 4
    spacing = jnp.exp(-jnp.log(10000.0) * jnp.arange(quarter, dtype=jnp.float32) / quarter)
    angles = positions.astype(jnp.float32)[:, None] * spacing[None, :]
    cosine_rows = jnp.cos(angles)
    sine_rows = jnp.sin(angles)
    first_part = key_rows[:, :quarter]
    second_part = key_rows[:, quarter : 2 * quarter]
    return jnp.concatenate(
        [
            first_part * cosine_rows - second_part * sine_rows,
            second_part * cosine_rows + first_part * sine_rows,
            key_rows[:, 2 * quarter :],
        ],
        axis=1,
    )


def fold_pairs(keep_rate, push_term):
    while keep_rate.shape[0] > 1:
        half_len = keep_rate.shape[0] // 2
        keep_pair = keep_rate.reshape(half_len, 2, keep_rate.shape[1])
        push_pair = push_term.reshape(half_len, 2, push_term.shape[1])
        push_term = keep_pair[:, 1] * push_pair[:, 0] + push_pair[:, 1]
        keep_rate = keep_pair[:, 0] * keep_pair[:, 1]
    return (keep_rate, push_term)


def on_device(
    tokens, attn_in, lengths, norm_gain, attn_gain, w_x, conv_w, w_a, w_i, lru_decay, w_kv
):
    local_len = tokens.shape[1]
    feature_dim = tokens.shape[2]
    seq_parts = lax.axis_size("seq")
    seq_place = lax.axis_index("seq")
    length = lengths[0]
    normed = rms_norm(tokens[0], norm_gain)
    projected = jnp.dot(
        normed,
        lax.all_gather(w_x, ("batch", "seq"), axis=0, tiled=True),
        preferred_element_type=jnp.float32,
    )
    x_proj = projected.astype(jnp.bfloat16)
    earlier_rows = passed_along(x_proj[local_len - 3 :], "seq", 1)
    padded = jnp.concatenate([earlier_rows, x_proj], axis=0)
    conv_sum = conv_w[0] * padded[0:local_len].astype(jnp.float32)
    for offset in range(1, 4):
        conv_sum = conv_sum + conv_w[offset] * padded[offset : offset + local_len].astype(
            jnp.float32
        )
    x_conv = conv_sum.astype(jnp.bfloat16)
    head_rows = x_conv.reshape(local_len, H, HD)
    gate_a = jnp.einsum("chk,hkj->chj", head_rows, w_a, preferred_element_type=jnp.float32).reshape(
        local_len, feature_dim
    )
    gate_i = jnp.einsum("chk,hkj->chj", head_rows, w_i, preferred_element_type=jnp.float32).reshape(
        local_len, feature_dim
    )
    positions = seq_place * local_len + jnp.arange(local_len, dtype=jnp.int32)
    valid_row = (positions < length).astype(jnp.float32)[:, None]
    log_rate = -8.0 * jax.nn.softplus(-lru_decay) * jax.nn.sigmoid(gate_a)
    keep_rate = jnp.exp(log_rate * valid_row)
    push_term = (
        jnp.sqrt(-jnp.expm1(2.0 * log_rate))
        * jax.nn.sigmoid(gate_i)
        * x_conv.astype(jnp.float32)
        * valid_row
    )
    keep_total, push_total = fold_pairs(keep_rate, push_term)
    wanted = length - 3 + jnp.arange(3, dtype=jnp.int32)
    picker = (positions[None, :] == wanted[:, None]).astype(jnp.bfloat16)
    conv_pick = jnp.dot(picker, x_proj, preferred_element_type=jnp.float32)
    lru_shard = jnp.zeros((feature_dim // seq_parts,), jnp.float32)
    summaries = (
        lax.all_to_all(keep_total, "seq", split_axis=1, concat_axis=0, tiled=True),
        lax.all_to_all(push_total, "seq", split_axis=1, concat_axis=0, tiled=True),
    )

    def advance(carried, step_pair):
        return (step_pair[0] * carried + step_pair[1], None)

    lru_shard = lax.scan(advance, lru_shard, summaries)[0]
    decoded = lax.psum_scatter(
        conv_pick[None].astype(jnp.bfloat16), "seq", scatter_dimension=2, tiled=True
    )
    lru_state = lru_shard[None]
    attn_normed = rms_norm(attn_in[0], attn_gain)
    kv_full = jnp.dot(attn_normed, w_kv, preferred_element_type=jnp.float32)
    kv_rows = jnp.concatenate(
        [rotate_keys(kv_full[:, :HD], positions), kv_full[:, HD:]], axis=1
    ).astype(jnp.bfloat16)
    in_window = ((positions >= length - W) & (positions < length)).astype(jnp.float32)[:, None]
    masked = kv_rows.astype(jnp.float32) * in_window
    slot_start = seq_place * local_len % W
    slot_buffer = lax.dynamic_update_slice(
        jnp.zeros((W, 2 * HD), jnp.float32), masked, (slot_start, jnp.int32(0))
    )
    kv_cache = lax.psum_scatter(
        slot_buffer.astype(jnp.bfloat16), "seq", scatter_dimension=1, tiled=True
    )
    return (lru_state, decoded, kv_cache[None])


def fits_two_cores(mesh):
    return mesh.shape["seq"] == 2 and mesh.shape["batch"] % 4 == 0 and mesh.shape["batch"] > 4


def solution(mesh):
    step = shared_by_cores if fits_two_cores(mesh) else on_device
    in_specs = (
        P("batch", "seq", None),
        P("batch", "seq", None),
        P("batch"),
        P(),
        P(),
        P(("batch", "seq"), None),
        P(),
        P(),
        P(),
        P(),
        P(),
    )
    out_specs = (P("batch", "seq"), P("batch", None, "seq"), P("batch", None, "seq"))
    return jax.shard_map(
        step, mesh=mesh, in_specs=in_specs, out_specs=out_specs, check_vma=False
    )
```
